32 devices in a mesh: dp: 8 (over z, y), tp: 4 (over x, core).
Axes of the slice: x: 2, y: 2, z: 4, core: 2. Of those that a mesh axis runs over, the one named last changes fastest.
Arguments:
- queries: bfloat16 [2048, 4096], P('dp', 'tp'), may hold values from -6 to 6
- keys: bfloat16 [2048, 512], P(('dp', 'tp')), may hold values from -6 to 6
- values: bfloat16 [2048, 512], P(('dp', 'tp')), may hold values from -6 to 6
- out_weight: bfloat16 [4096, 8192], P('tp', 'dp'), may hold values from -0.09375 to 0.09375
- residual: bfloat16 [2048, 8192], P(('dp', 'tp')), may hold values from -40 to 40
- norm_gain: float32 [8192], replicated, may hold values from 0.5 to 1.5
Outputs:
- hidden_out: bfloat16 [2048, 8192], P(('dp', 'tp'))
- normed: bfloat16 [2048, 8192], P(('dp', 'tp'))
The draws below stay inside these ranges and needn't reach their ends.
All inputs are finite; a program needn't handle non-finite values.
Results may differ from the reference program's by a relative error of at most 0.012.
Values may be sent and summed in bfloat16 or wider, within the bound.
A program may use at most 64 MiB of HBM per device.

```python
import math
import jax
import jax.numpy as jnp
from jax import lax

D = 8192
HQ = 32
KVH = 4
HDIM = 128
LEN = 32
TOKENS = 2048
N_TP = 4


def draw_queries(key, part):
    base = jax.random.truncated_normal(jax.random.fold_in(key, 1), -6.0, 6.0, (TOKENS, HQ * HDIM), jnp.float32)
    return base.astype(jnp.bfloat16)


def draw_keys(key, part):
    base = jax.random.truncated_normal(jax.random.fold_in(key, 2), -6.0, 6.0, (TOKENS, KVH * HDIM), jnp.float32)
    return base.astype(jnp.bfloat16)


def draw_residual(key, part):
    base = jax.random.truncated_normal(jax.random.fold_in(key, 3), -6.0, 6.0, (TOKENS, D), jnp.float32)
    lowest = 0.08
    row_scale = jnp.exp(jax.random.uniform(jax.random.fold_in(key, 4), (TOKENS, 1), jnp.float32, math.log(lowest), math.log(10.0 * lowest)))
    column_scale = jnp.exp(jax.random.uniform(jax.random.fold_in(key, 5), (1, D), jnp.float32, math.log(0.35), math.log(3.5)))
    return jnp.clip(base * row_scale * column_scale, -40.0, 40.0).astype(jnp.bfloat16)


def level_of(rng, dims, shards, least, largest):
    loudness = 1.0
    for axis_at, blocks in shards:
        heights = jax.random.uniform(jax.random.fold_in(jax.random.fold_in(rng, 6), axis_at), (blocks,), jnp.float32, least / len(shards), largest / len(shards))
        loudness = loudness * jnp.repeat(jnp.exp(heights), dims[axis_at] // blocks).reshape((-1,) + (1,) * (len(dims) - 1 - axis_at))
    return loudness


def noise(rng, shape, scale, reach, cuts=(), held_as=jnp.bfloat16):
    factor_of = level_of(rng, shape, cuts, -0.22, 0.18) if cuts else 1.0
    result = jax.random.normal(rng, shape, jnp.float32) * scale * factor_of
    return jnp.minimum(jnp.maximum(result, -reach), reach).astype(held_as)


def setup_inputs(seed: int = 0) -> dict:
    key_of = jax.random.split(jax.random.key(seed), 7)
    return {
        "queries": draw_queries(jax.random.fold_in(key_of[6], 71), 0),
        "keys": draw_keys(jax.random.fold_in(key_of[6], 71), 0),
        "values": noise(key_of[2], (TOKENS, KVH * HDIM), 1.0, 6.0, ((0, 32),)),
        "out_weight": noise(key_of[3], (HQ * HDIM, D), (HQ * HDIM) ** -0.5, 0.09375, ((0, 4), (1, 8))),
        "residual": draw_residual(jax.random.fold_in(key_of[6], 71), 0),
        "norm_gain": jnp.clip(1.0 + 0.1 * jax.random.normal(key_of[5], (D,), jnp.float32), 0.5, 1.5),
    }


def attend(queries, keys, values):
    sequences = queries.shape[0] // LEN
    group = HQ // KVH
    query_heads = queries.reshape(sequences, LEN, HQ, HDIM).astype(jnp.float32)
    key_heads = jnp.repeat(keys.reshape(sequences, LEN, KVH, HDIM).astype(jnp.float32), group, axis=2)
    value_heads = jnp.repeat(values.reshape(sequences, LEN, KVH, HDIM).astype(jnp.float32), group, axis=2)
    scores = jnp.einsum('slhd,smhd->shlm', query_heads, key_heads) / math.sqrt(HDIM)
    causal = jnp.arange(LEN)[:, None] >= jnp.arange(LEN)[None, :]
    scores = jnp.where(causal, scores, -1e+30)
    highest = lax.optimization_barrier(jnp.max(scores, axis=-1, keepdims=True))
    powers = jnp.exp(scores - highest)
    weights = (powers / lax.optimization_barrier(jnp.sum(powers, axis=-1, keepdims=True))).astype(jnp.bfloat16)
    attended = jnp.einsum('shlm,smhd->slhd', weights.astype(jnp.float32), value_heads)
    return attended.astype(jnp.bfloat16).reshape(queries.shape[0], HQ * HDIM)

def reference(queries, keys, values, out_weight, residual, norm_gain):
    attended = attend(queries, keys, values)
    width = HQ * HDIM // N_TP
    projected = jnp.zeros((queries.shape[0], D), jnp.float32)
    for block in range(N_TP):
        term = jnp.dot(attended[:, block * width:(block + 1) * width], out_weight[block * width:(block + 1) * width], preferred_element_type=jnp.float32)
        rounded = lax.optimization_barrier(term.astype(jnp.bfloat16))
        projected = projected + rounded.astype(jnp.float32)
    updated = residual.astype(jnp.float32) + projected
    hidden_out = updated.astype(jnp.bfloat16)
    meansq = lax.optimization_barrier(jnp.mean(updated * updated, axis=-1, keepdims=True))
    normed = (updated * lax.rsqrt(meansq + 1e-05) * norm_gain).astype(jnp.bfloat16)
    return (hidden_out, normed)
```

```python
import functools
import math

import jax
import jax.numpy as jnp
from jax import lax
from jax.experimental import pallas as pl
from jax.experimental.pallas import tpu as pltpu
from jax.sharding import PartitionSpec as P

KVH = 4
HDIM = 128
LEN = 32
MESH = pl.DeviceIdType.MESH
BF = jnp.bfloat16
F32 = jnp.float32


def flip(value, mask, bits):
    for bit in range(bits):
        step = 1 << bit
        if mask & step:
            value = value + step - 2 * step * ((value // step) % 2)
    return value


def reverse(value, bits):
    return sum(((value >> bit) & 1) << (bits - 1 - bit) for bit in range(bits))


def pick(index, table):
    result = jnp.int32(table[0])
    for at, entry in enumerate(table[1:], 1):
        result = jnp.where(index == at, jnp.int32(entry), result)
    return result


def visit_order(at, line):
    return sorted(range(line), key=lambda other: (abs(other - at), (other > at) == (at * 2 < line - 1)))


def plan(line, blocks, pieces, halves, stages):
    hop, start, weights = 11.0, 8.0, 42.0
    events = []
    for k in range(1, line):
        for half in range(halves):
            distance = (k + 1) // 2
            events.append((start + hop * (distance - 1) + hop * (half + 1) / halves, 0, ("forward", k, half)))
    units = []
    for k in range(line):
        for c in range(blocks * pieces):
            there = 0.0 if c < pieces else 3.0 + weights * (c - pieces + 1) / (blocks * pieces - pieces)
            units.append((max(start + hop * k, there), k, c))
    units.sort()
    clock = 0.0
    for number, (when, k, c) in enumerate(units):
        clock = max(when, clock + 0.7)
        events.append((clock, 1, ("unit", number, 0)))
        for stage in range(1, stages + 1):
            events.append((clock + (1.5 if stage == 1 else 1.5 + 2.5 * (stage - 1)), 2 + stage, ("stage", number, stage)))
    events.sort()
    return [(k, c) for _, k, c in units], [event for _, _, event in events]


def kernel(cfg, q_ref, k_ref, v_ref, w_ref, r_ref, g_ref, hid_ref, nrm_ref,
           q_v, k_v, v_v, att, w_v, r_v, g_v, keeps, sends, recvs, fin, fin_snd, upd, hid_v, nrm_v,
           loc_sem, kv_snd, kv_rcv, g_snd, g_rcv, w_snd, w_rcv, s_snd, s_rcv, f_snd, f_rcv, o_sem):
    tp, dp, line, blocks, pieces, halves, stages = cfg
    rows, width = q_v.shape
    cols = w_v.shape[2]
    own_cols = cols * pieces
    tok = rows // tp
    features = fin.shape[1]
    me_dp, me = lax.axis_index("dp"), lax.axis_index("tp")
    a, b = me_dp // blocks, me_dp % blocks
    slot = [reverse(i, stages) for i in range(tp)]

    def dev(aa, bb, tt):
        return (aa * blocks + bb, tt)

    def remote(src, dst, snd, rcv, device):
        return pltpu.make_async_remote_copy(
            src_ref=src, dst_ref=dst, send_sem=snd, recv_sem=rcv, device_id=device, device_id_type=MESH)

    def aligned(value, unit):
        return pl.ds(pl.multiple_of(value, unit), unit)

    locals_ = []

    def local(src, dst):
        copy = pltpu.make_async_copy(src, dst, loc_sem.at[len(locals_)])
        copy.start()
        locals_.append(copy)
        return copy

    head = me * KVH // tp
    first = []
    for i in range(tp):
        first.append(local(q_ref.at[aligned(flip(me, i, stages) * tok, tok)], q_v.at[pl.ds(slot[i] * tok, tok)]))
    first.append(local(k_ref.at[:, aligned(head * HDIM, HDIM)], k_v.at[pl.ds(0, tok)]))
    first.append(local(v_ref.at[:, aligned(head * HDIM, HDIM)], v_v.at[pl.ds(0, tok)]))
    w_local = [local(w_ref.at[:, pl.ds(s * cols, cols)], w_v.at[s]) for s in range(pieces)]
    r_local = [local(r_ref, r_v), local(g_ref, g_v)]

    barrier = pltpu.get_barrier_semaphore()
    order = [pick(a, [visit_order(at, line)[k] for at in range(line)]) for k in range(line)]
    for i in range(1, tp):
        pl.semaphore_signal(barrier, inc=1, device_id=dev(a, b, flip(me, i, stages)), device_id_type=MESH)
    for j in range(1, blocks):
        pl.semaphore_signal(barrier, inc=1, device_id=dev(a, (b + j) % blocks, me), device_id_type=MESH)
    for k in range(1, line):
        pl.semaphore_signal(barrier, inc=1, device_id=dev(order[k], b, me), device_id_type=MESH)
    pl.semaphore_wait(barrier, tp - 1 + blocks - 1 + line - 1)

    kv = []
    for i in range(1, tp):
        peer = flip(me, i, stages)
        lanes = aligned((peer * KVH // tp) * HDIM, HDIM)
        for n, (src, dst) in enumerate(((k_ref, k_v), (v_ref, v_v))):
            copy = remote(src.at[:, lanes], dst.at[pl.ds(slot[i] * tok, tok)],
                          kv_snd.at[n, i], kv_rcv.at[n, i], dev(a, b, peer))
            copy.start()
            kv.append(copy)

    w_copies = {}
    for j in range(1, blocks):
        for s in range(pieces):
            c = j * pieces + s
            copy = remote(w_ref.at[:, pl.ds(s * cols, cols)], w_v.at[c], w_snd.at[c], w_rcv.at[c],
                          dev(a, (b + blocks - j) % blocks, me))
            copy.start()
            w_copies[c] = copy

    for copy in first:
        copy.wait()
    for copy in kv:
        copy.wait_recv()

    size = rows // halves
    heads = width // HDIM

    def token(index):
        block = index // tok
        where = jnp.zeros_like(index)
        for bit in range(stages):
            mine = (me // (1 << bit)) % 2
            theirs = (block // (1 << (stages - 1 - bit))) % 2
            where = where + (1 << bit) * ((mine + theirs) % 2)
        return where * tok + index % tok

    def att_part(source, half):
        return att.at[source, pl.ds(half * size, size)]

    def hop(source, half, target, way):
        part = att_part(source, half)
        return remote(part, part, g_snd.at[source, half, way], g_rcv.at[source, half], dev(target, b, me))

    def line_send(source, half, down, up):
        @pl.when(down)
        def _():
            hop(source, half, a - 1, 0).start()

        @pl.when(up)
        def _():
            hop(source, half, a + 1, 1).start()

    for half in range(halves):
        part = pl.ds(half * size, size)
        row = lax.broadcasted_iota(jnp.int32, (size, size), 0)
        col = lax.broadcasted_iota(jnp.int32, (size, size), 1)
        if tok % LEN:
            row, col = token(row + half * size), token(col + half * size)
        seen = (row // LEN == col // LEN) & (row >= col)
        keys, vals = k_v[part, :], v_v[part, :]
        for h in range(heads):
            lanes = pl.ds(h * HDIM, HDIM)
            scores = lax.dot_general(q_v[part, lanes], keys, (((1,), (1,)), ((), ())),
                                     preferred_element_type=F32) / math.sqrt(HDIM)
            scores = jnp.where(seen, scores, -1e30)
            powers = jnp.exp(scores - jnp.max(scores, axis=-1, keepdims=True))
            probs = (powers / jnp.sum(powers, axis=-1, keepdims=True)).astype(BF)
            att[a, part, lanes] = jnp.dot(probs, vals, preferred_element_type=F32).astype(BF)
        line_send(a, half, a > 0, a < line - 1)

    for copy in w_local:
        copy.wait()

    units, events = plan(line, blocks, pieces, halves, stages)
    have_w, have_k = set(range(pieces)), {0}

    def passes(k):
        source = order[k]
        down = jnp.logical_and(source > a, a > 0)
        up = jnp.logical_and(source < a, a < line - 1)
        return source, down, up

    def finish(number, total):
        k, c = units[number]
        j, s = divmod(c, pieces)
        start = (a * blocks + (b + j) % blocks) * own_cols + s * cols
        lanes = aligned(start, cols)
        if k == 0:
            fin[:, lanes] = total.astype(BF)
            return
        fin_snd[number] = total.astype(BF)
        remote(fin_snd.at[number], fin.at[:, lanes], f_snd.at[number], f_rcv.at[a, c], dev(order[k], b, me)).start()

    def exchange(number, stage):
        return remote(sends[stage].at[number], recvs[stage].at[number], s_snd.at[stage, number],
                      s_rcv.at[stage, number], dev(a, b, flip(me, 1 << stage, stages)))

    def pass_on(number, stage, total):
        if stage == stages:
            finish(number, total)
            return
        mid = total.shape[0] // 2
        sends[stage][number] = total[mid:].astype(BF)
        exchange(number, stage).start()
        keeps[stage][number] = total[:mid]

    for kind, number, extra in events:
        if kind == "forward":
            source, down, up = passes(number)

            @pl.when(jnp.logical_or(down, up))
            def _():
                hop(source, extra, a, 0).wait_recv()

            line_send(source, extra, down, up)
        elif kind == "unit":
            k, c = units[number]
            source, down, up = passes(k)
            if k not in have_k:
                have_k.add(k)

                @pl.when(jnp.logical_not(jnp.logical_or(down, up)))
                def _():
                    for half in range(halves):
                        hop(source, half, a, 0).wait_recv()

            if c not in have_w:
                have_w.add(c)
                w_copies[c].wait_recv()
            pass_on(number, 0, jnp.dot(att[source], w_v[c], preferred_element_type=F32))
        else:
            exchange(number, extra - 1).wait_recv()
            total = keeps[extra - 1][number] + recvs[extra - 1][number].astype(F32)
            pass_on(number, extra, total)

    for copy in r_local:
        copy.wait()
    squares = jnp.zeros((tok, 1), F32)

    for k in range(line):
        source = order[k]
        for c in range(blocks * pieces):
            j, s = divmod(c, pieces)
            lanes = aligned((source * blocks + (b + j) % blocks) * own_cols + s * cols, cols)
            if k:
                remote(fin.at[:, lanes], fin.at[:, lanes], f_snd.at[0], f_rcv.at[source, c],
                       dev(source, b, me)).wait_recv()
            now = r_v[:, lanes].astype(F32) + fin[:, lanes].astype(F32)
            upd[:, lanes] = now
            hid_v[:, lanes] = now.astype(BF)
            squares = squares + jnp.sum(now * now, axis=-1, keepdims=True)
    out_h = pltpu.make_async_copy(hid_v, hid_ref, o_sem.at[0])
    out_h.start()
    scale = lax.rsqrt(squares / features + 1e-05)
    step = min(features, 1024)
    for n in range(features // step):
        lanes = pl.ds(n * step, step)
        nrm_v[:, lanes] = (upd[:, lanes] * scale * g_v[:, lanes]).astype(BF)
    out_n = pltpu.make_async_copy(nrm_v, nrm_ref, o_sem.at[1])
    out_n.start()

    for copy in kv:
        copy.wait_send()
    for copy in w_copies.values():
        copy.wait_send()
    for k in range(line):
        if k:
            source, down, up = passes(k)
        else:
            source, down, up = a, a > 0, a < line - 1
        for half in range(halves):
            @pl.when(down)
            def _():
                hop(source, half, a - 1, 0).wait_send()

            @pl.when(up)
            def _():
                hop(source, half, a + 1, 1).wait_send()
    for number, (k, c) in enumerate(units):
        for stage in range(stages):
            exchange(number, stage).wait_send()
        if k:
            remote(fin_snd.at[number], fin.at[:, pl.ds(0, cols)], f_snd.at[number], f_rcv.at[a, c],
                   dev(order[k], b, me)).wait_send()
    out_h.wait()
    out_n.wait()


def local(tp, dp, queries, keys, values, out_weight, residual, norm_gain):
    rows, width = queries.shape
    own_cols = out_weight.shape[1]
    tok, features = residual.shape
    blocks = 2 if dp % 2 == 0 else 1
    line = dp // blocks
    pieces = max(1, min(2, own_cols // 256))
    cols = own_cols // pieces
    halves = 2 if tok % LEN == 0 else 1
    stages = tp.bit_length() - 1
    chunks = blocks * pieces
    count = line * chunks
    any_ = pl.BlockSpec(memory_space=pl.ANY)
    vm = pltpu.VMEM
    dma = pltpu.SemaphoreType.DMA
    cfg = (tp, dp, line, blocks, pieces, halves, stages)
    parts = [rows >> (stage + 1) for stage in range(stages)]
    out = jax.ShapeDtypeStruct((tok, features), BF)
    return pl.pallas_call(
        functools.partial(kernel, cfg),
        out_shape=(out, out),
        in_specs=[any_] * 6,
        out_specs=(any_, any_),
        scratch_shapes=[
            vm((rows, width), BF), vm((rows, HDIM), BF), vm((rows, HDIM), BF),
            vm((line, rows, width), BF), vm((chunks, width, cols), BF),
            vm((tok, features), BF), vm((1, features), F32),
            tuple(vm((count, part, cols), F32) for part in parts),
            tuple(vm((count, part, cols), BF) for part in parts),
            tuple(vm((count, part, cols), BF) for part in parts),
            vm((tok, features), BF), vm((count, tok, cols), BF), vm((tok, features), F32),
            vm((tok, features), BF), vm((tok, features), BF),
            dma((tp + 4 + pieces,)), dma((2, tp)), dma((2, tp)),
            dma((line, halves, 2)), dma((line, halves)), dma((chunks,)), dma((chunks,)),
            dma((stages, count)), dma((stages, count)), dma((count,)), dma((line, chunks)), dma((2,)),
        ],
        compiler_params=pltpu.CompilerParams(
            collective_id=0, has_side_effects=True, vmem_limit_bytes=56 * 1024 * 1024),
    )(queries, keys, values, out_weight, residual, norm_gain.reshape(1, features))


def solution(mesh):
    return jax.shard_map(
        functools.partial(local, mesh.shape["tp"], mesh.shape["dp"]),
        mesh=mesh,
        in_specs=(
            P("dp", "tp"),
            P(("dp", "tp"), None),
            P(("dp", "tp"), None),
            P("tp", "dp"),
            P(("dp", "tp"), None),
            P(),
        ),
        out_specs=(P(("dp", "tp"), None), P(("dp", "tp"), None)),
        check_vma=False,
    )
```

```python
import functools
import math

import jax
import jax.numpy as jnp
from jax import lax
from jax.experimental import pallas as pl
from jax.experimental.pallas import tpu as pltpu
from jax.sharding import PartitionSpec as P

KVH = 4
HDIM = 128
LEN = 32
MESH = pl.DeviceIdType.MESH
BF = jnp.bfloat16
F32 = jnp.float32


def flip(value, mask, bits):
    for bit in range(bits):
        step = 1 << bit
        if mask & step:
            value = value + step - 2 * step * ((value // step) % 2)
    return value


def reverse(value, bits):
    return sum(((value >> bit) & 1) << (bits - 1 - bit) for bit in range(bits))


def pick(index, table):
    result = jnp.int32(table[0])
    for at, entry in enumerate(table[1:], 1):
        result = jnp.where(index == at, jnp.int32(entry), result)
    return result


def visit_order(at, line):
    return sorted(range(line), key=lambda other: (abs(other - at), (other > at) == (at * 2 < line - 1)))


def plan(line, blocks, pieces, halves, stages):
    hop, start, weights = 11.0, 8.0, 42.0
    events = []
    for k in range(1, line):
        for half in range(halves):
            distance = (k + 1) // 2
            events.append((start + hop * (distance - 1) + hop * (half + 1) / halves, 0, ("forward", k, half)))
    units = []
    for k in range(line):
        for c in range(blocks * pieces):
            there = 0.0 if c < pieces else 3.0 + weights * (c - pieces + 1) / (blocks * pieces - pieces)
            units.append((max(start + hop * k, there), k, c))
    units.sort()
    clock = 0.0
    for number, (when, k, c) in enumerate(units):
        clock = max(when, clock + 0.7)
        events.append((clock, 1, ("unit", number, 0)))
        for stage in range(1, stages + 1):
            events.append((clock + (1.5 if stage == 1 else 1.5 + 2.5 * (stage - 1)), 2 + stage, ("stage", number, stage)))
    events.sort()
    return [(k, c) for _, k, c in units], [event for _, _, event in events]


def kernel(cfg, q_ref, k_ref, v_ref, w_ref, out_ref,
           q_v, k_v, v_v, att, w_v, keeps, sends, recvs, fin_snd,
           loc_sem, kv_snd, kv_rcv, g_snd, g_rcv, w_snd, w_rcv, s_snd, s_rcv, f_snd, f_rcv):
    tp, dp, line, blocks, pieces, halves, stages = cfg
    rows, width = q_v.shape
    cols = w_v.shape[2]
    own_cols = cols * pieces
    tok = rows // tp
    me_dp, me = lax.axis_index("dp"), lax.axis_index("tp")
    a, b = me_dp // blocks, me_dp % blocks
    slot = [reverse(i, stages) for i in range(tp)]

    def dev(aa, bb, tt):
        return (aa * blocks + bb, tt)

    def remote(src, dst, snd, rcv, device):
        return pltpu.make_async_remote_copy(
            src_ref=src, dst_ref=dst, send_sem=snd, recv_sem=rcv, device_id=device, device_id_type=MESH)

    def aligned(value, unit):
        return pl.ds(pl.multiple_of(value, unit), unit)

    locals_ = []

    def local(src, dst):
        copy = pltpu.make_async_copy(src, dst, loc_sem.at[len(locals_)])
        copy.start()
        locals_.append(copy)
        return copy

    head = me * KVH // tp
    first = []
    for i in range(tp):
        first.append(local(q_ref.at[aligned(flip(me, i, stages) * tok, tok)], q_v.at[pl.ds(slot[i] * tok, tok)]))
    first.append(local(k_ref.at[:, aligned(head * HDIM, HDIM)], k_v.at[pl.ds(0, tok)]))
    first.append(local(v_ref.at[:, aligned(head * HDIM, HDIM)], v_v.at[pl.ds(0, tok)]))
    w_local = [local(w_ref.at[:, pl.ds(s * cols, cols)], w_v.at[s]) for s in range(pieces)]

    barrier = pltpu.get_barrier_semaphore()
    order = [pick(a, [visit_order(at, line)[k] for at in range(line)]) for k in range(line)]
    for i in range(1, tp):
        pl.semaphore_signal(barrier, inc=1, device_id=dev(a, b, flip(me, i, stages)), device_id_type=MESH)
    for j in range(1, blocks):
        pl.semaphore_signal(barrier, inc=1, device_id=dev(a, (b + j) % blocks, me), device_id_type=MESH)
    for k in range(1, line):
        pl.semaphore_signal(barrier, inc=1, device_id=dev(order[k], b, me), device_id_type=MESH)
    pl.semaphore_wait(barrier, tp - 1 + blocks - 1 + line - 1)

    kv = []
    for i in range(1, tp):
        peer = flip(me, i, stages)
        lanes = aligned((peer * KVH // tp) * HDIM, HDIM)
        for n, (src, dst) in enumerate(((k_ref, k_v), (v_ref, v_v))):
            copy = remote(src.at[:, lanes], dst.at[pl.ds(slot[i] * tok, tok)],
                          kv_snd.at[n, i], kv_rcv.at[n, i], dev(a, b, peer))
            copy.start()
            kv.append(copy)

    w_copies = {}
    for j in range(1, blocks):
        for s in range(pieces):
            c = j * pieces + s
            copy = remote(w_ref.at[:, pl.ds(s * cols, cols)], w_v.at[c], w_snd.at[c], w_rcv.at[c],
                          dev(a, (b + blocks - j) % blocks, me))
            copy.start()
            w_copies[c] = copy

    for copy in first:
        copy.wait()
    for copy in kv:
        copy.wait_recv()

    size = rows // halves
    heads = width // HDIM

    def token(index):
        block = index // tok
        where = jnp.zeros_like(index)
        for bit in range(stages):
            mine = (me // (1 << bit)) % 2
            theirs = (block // (1 << (stages - 1 - bit))) % 2
            where = where + (1 << bit) * ((mine + theirs) % 2)
        return where * tok + index % tok

    def att_part(source, half):
        return att.at[source, pl.ds(half * size, size)]

    def hop(source, half, target, way):
        part = att_part(source, half)
        return remote(part, part, g_snd.at[source, half, way], g_rcv.at[source, half], dev(target, b, me))

    def line_send(source, half, down, up):
        @pl.when(down)
        def _():
            hop(source, half, a - 1, 0).start()

        @pl.when(up)
        def _():
            hop(source, half, a + 1, 1).start()

    for half in range(halves):
        part = pl.ds(half * size, size)
        row = lax.broadcasted_iota(jnp.int32, (size, size), 0)
        col = lax.broadcasted_iota(jnp.int32, (size, size), 1)
        if tok % LEN:
            row, col = token(row + half * size), token(col + half * size)
        seen = (row // LEN == col // LEN) & (row >= col)
        keys, vals = k_v[part, :], v_v[part, :]
        for h in range(heads):
            lanes = pl.ds(h * HDIM, HDIM)
            scores = lax.dot_general(q_v[part, lanes], keys, (((1,), (1,)), ((), ())),
                                     preferred_element_type=F32) / math.sqrt(HDIM)
            scores = jnp.where(seen, scores, -1e30)
            powers = jnp.exp(scores - jnp.max(scores, axis=-1, keepdims=True))
            probs = (powers / jnp.sum(powers, axis=-1, keepdims=True)).astype(BF)
            att[a, part, lanes] = jnp.dot(probs, vals, preferred_element_type=F32).astype(BF)
        line_send(a, half, a > 0, a < line - 1)

    for copy in w_local:
        copy.wait()

    units, events = plan(line, blocks, pieces, halves, stages)
    have_w, have_k = set(range(pieces)), {0}

    def passes(k):
        source = order[k]
        down = jnp.logical_and(source > a, a > 0)
        up = jnp.logical_and(source < a, a < line - 1)
        return source, down, up

    def finish(number, total):
        k, c = units[number]
        j, s = divmod(c, pieces)
        start = (a * blocks + (b + j) % blocks) * own_cols + s * cols
        lanes = aligned(start, cols)
        fin_snd[number] = total.astype(BF)
        if k == 0:
            pltpu.make_async_copy(fin_snd.at[number], out_ref.at[:, lanes], f_snd.at[number]).start()
        else:
            remote(fin_snd.at[number], out_ref.at[:, lanes], f_snd.at[number], f_rcv.at[a, c],
                   dev(order[k], b, me)).start()

    def exchange(number, stage):
        return remote(sends[stage].at[number], recvs[stage].at[number], s_snd.at[stage, number],
                      s_rcv.at[stage, number], dev(a, b, flip(me, 1 << stage, stages)))

    def pass_on(number, stage, total):
        if stage == stages:
            finish(number, total)
            return
        mid = total.shape[0] // 2
        sends[stage][number] = total[mid:].astype(BF)
        exchange(number, stage).start()
        keeps[stage][number] = total[:mid]

    for kind, number, extra in events:
        if kind == "forward":
            source, down, up = passes(number)

            @pl.when(jnp.logical_or(down, up))
            def _():
                hop(source, extra, a, 0).wait_recv()

            line_send(source, extra, down, up)
        elif kind == "unit":
            k, c = units[number]
            source, down, up = passes(k)
            if k not in have_k:
                have_k.add(k)

                @pl.when(jnp.logical_not(jnp.logical_or(down, up)))
                def _():
                    for half in range(halves):
                        hop(source, half, a, 0).wait_recv()

            if c not in have_w:
                have_w.add(c)
                w_copies[c].wait_recv()
            pass_on(number, 0, jnp.dot(att[source], w_v[c], preferred_element_type=F32))
        else:
            exchange(number, extra - 1).wait_recv()
            total = keeps[extra - 1][number] + recvs[extra - 1][number].astype(F32)
            pass_on(number, extra, total)

    for k in range(1, line):
        for c in range(blocks * pieces):
            remote(fin_snd.at[0], out_ref.at[:, pl.ds(0, cols)], f_snd.at[0], f_rcv.at[order[k], c],
                   dev(order[k], b, me)).wait_recv()

    for copy in kv:
        copy.wait_send()
    for copy in w_copies.values():
        copy.wait_send()
    for k in range(line):
        if k:
            source, down, up = passes(k)
        else:
            source, down, up = a, a > 0, a < line - 1
        for half in range(halves):
            @pl.when(down)
            def _():
                hop(source, half, a - 1, 0).wait_send()

            @pl.when(up)
            def _():
                hop(source, half, a + 1, 1).wait_send()
    for number, (k, c) in enumerate(units):
        for stage in range(stages):
            exchange(number, stage).wait_send()
        if k:
            remote(fin_snd.at[number], out_ref.at[:, pl.ds(0, cols)], f_snd.at[number], f_rcv.at[a, c],
                   dev(order[k], b, me)).wait_send()
        else:
            pltpu.make_async_copy(fin_snd.at[number], out_ref.at[:, pl.ds(0, cols)], f_snd.at[number]).wait()


def norm_kernel(p_ref, r_ref, g_ref, hid_ref, nrm_ref):
    updated = r_ref[...].astype(F32) + p_ref[...].astype(F32)
    hid_ref[...] = updated.astype(BF)
    scale = lax.rsqrt(jnp.mean(updated * updated, axis=-1, keepdims=True) + 1e-05)
    nrm_ref[...] = (updated * scale * g_ref[...]).astype(BF)


def local(tp, dp, queries, keys, values, out_weight, residual, norm_gain):
    rows, width = queries.shape
    own_cols = out_weight.shape[1]
    tok, features = residual.shape
    blocks = 2 if dp % 2 == 0 else 1
    line = dp // blocks
    pieces = max(1, min(4, own_cols // 256))
    cols = own_cols // pieces
    halves = 2 if tok % LEN == 0 else 1
    stages = tp.bit_length() - 1
    chunks = blocks * pieces
    count = line * chunks
    any_ = pl.BlockSpec(memory_space=pl.ANY)
    vm = pltpu.VMEM
    dma = pltpu.SemaphoreType.DMA
    cfg = (tp, dp, line, blocks, pieces, halves, stages)
    parts = [rows >> (stage + 1) for stage in range(stages)]
    out = jax.ShapeDtypeStruct((tok, features), BF)
    projected = pl.pallas_call(
        functools.partial(kernel, cfg),
        out_shape=out,
        in_specs=[any_] * 4,
        out_specs=any_,
        scratch_shapes=[
            vm((rows, width), BF), vm((rows, HDIM), BF), vm((rows, HDIM), BF),
            vm((line, rows, width), BF), vm((chunks, width, cols), BF),
            tuple(vm((count, part, cols), F32) for part in parts),
            tuple(vm((count, part, cols), BF) for part in parts),
            tuple(vm((count, part, cols), BF) for part in parts),
            vm((count, tok, cols), BF),
            dma((tp + 2 + pieces,)), dma((2, tp)), dma((2, tp)),
            dma((line, halves, 2)), dma((line, halves)), dma((chunks,)), dma((chunks,)),
            dma((stages, count)), dma((stages, count)), dma((count,)), dma((line, chunks)),
        ],
        compiler_params=pltpu.CompilerParams(
            collective_id=0, has_side_effects=True, vmem_limit_bytes=56 * 1024 * 1024),
    )(queries, keys, values, out_weight)
    high = min(16, tok)
    block = pl.BlockSpec((high, features), lambda i: (i, 0))
    return pl.pallas_call(
        norm_kernel,
        grid=(tok // high,),
        out_shape=(out, out),
        in_specs=[block, block, pl.BlockSpec((1, features), lambda i: (0, 0))],
        out_specs=(block, block),
    )(projected, residual, norm_gain.reshape(1, features))


def solution(mesh):
    return jax.shard_map(
        functools.partial(local, mesh.shape["tp"], mesh.shape["dp"]),
        mesh=mesh,
        in_specs=(
            P("dp", "tp"),
            P(("dp", "tp"), None),
            P(("dp", "tp"), None),
            P("tp", "dp"),
            P(("dp", "tp"), None),
            P(),
        ),
        out_specs=(P(("dp", "tp"), None), P(("dp", "tp"), None)),
        check_vma=False,
    )
```
